256 devices in a mesh: dp: 128 (over y, x_lo, z, core), rep: 2 (over x_hi).
Axes of the slice: x: 4 (x_hi: 2, x_lo: 2; x = x_hi * 2 + x_lo), y: 4, z: 8, core: 2. Of those that a mesh axis runs over, the one named last changes fastest.
Arguments:
- q_hidden: bfloat16 [2, 128, 128, 768], P('rep', 'dp'), may hold values from -8 to 8
- p_hidden: bfloat16 [2, 128, 128, 768], P('rep', 'dp'), may hold values from -8 to 8
- w_up: bfloat16 [1536, 768], replicated, may hold values from -0.21875 to 0.21875
- w_down: bfloat16 [1536, 768], replicated, may hold values from -0.15625 to 0.15625
- pos_index: int32 [2, 128], P('rep', 'dp'), may hold values from 0 to 127
- hard_index: int32 [2, 128, 2], P('rep', 'dp'), may hold values from 0 to 127
Outputs:
- w_up_grad: float32 [1536, 768], P(('dp', 'rep'))
- mean_loss: float32 [], replicated
The draws below stay inside these ranges and needn't reach their ends.
All inputs are finite; a program needn't handle non-finite values.
Results may differ from the reference program's by a relative error of at most 0.008.
Values may be sent and summed in bfloat16 or wider, within the bound.
No kernel may reach another device: no remote copies, remote signals or barrier semaphores. Data moves between devices by JAX's collectives and lax.ppermute only.
A program may use at most 64 MiB of HBM per device.

```python
import math
import jax
import jax.numpy as jnp
from jax import lax

D = 768
FF = 1536
LEN = 128
HARD = 2
REPLICAS = 2
GQ = 128
GP = 128


def hidden_pair(key):
    shape = (2, REPLICAS, GQ, LEN, D)
    topic = jax.random.normal(jax.random.fold_in(key, 101), (2, REPLICAS, GQ, 1, D), jnp.float32)
    noise = jax.random.normal(jax.random.fold_in(key, 202), shape, jnp.float32)
    both = 0.35 * topic + noise
    return jnp.clip(both, -8.0, 8.0)


def draw_q_hidden(key, part):
    return hidden_pair(key)[0].astype(jnp.bfloat16)


def draw_p_hidden(key, part):
    return hidden_pair(key)[1].astype(jnp.bfloat16)


def place_ends(array, stream_key, low, top_value):
    dims = array.shape
    spot = [jax.random.randint(jax.random.fold_in(stream_key, axis), (), 0, dims[axis]) for axis in range(len(dims))]
    array = array.at[tuple(spot)].set(low)
    longest = dims.index(max(dims))
    spot[longest] = (spot[longest] + 1) % dims[longest]
    return array.at[tuple(spot)].set(top_value)


def normal_values(rng, shape, width, reach, kind=jnp.bfloat16):
    return jnp.clip(width * jax.random.normal(rng, shape, jnp.float32), -reach, reach).astype(kind)


def setup_inputs(seed: int = 0) -> dict:
    keys = jax.random.split(jax.random.key(seed), 7)
    return {
        "q_hidden": draw_q_hidden(jax.random.fold_in(keys[6], 71), 0),
        "p_hidden": draw_p_hidden(jax.random.fold_in(keys[6], 71), 0),
        "w_up": normal_values(keys[2], (FF, D), D ** -0.5, 0.21875),
        "w_down": normal_values(keys[3], (FF, D), FF ** -0.5, 0.15625),
        "pos_index": place_ends(jax.random.randint(keys[4], (REPLICAS, GQ), 0, GP), jax.random.fold_in(keys[4], 1), 0, GP - 1).astype(jnp.int32),
        "hard_index": place_ends(jax.random.randint(keys[5], (REPLICAS, GQ, HARD), 0, GP), jax.random.fold_in(keys[5], 1), 0, GP - 1).astype(jnp.int32),
    }


norm_eps = 1e-06
HARD_BOOST = 1.5

def gelu_slope(values):
    cdf_part = 0.5 * (1.0 + lax.erf(values * (1.0 / math.sqrt(2.0))))
    return cdf_part + values * jnp.exp(-0.5 * values * values) * (1.0 / math.sqrt(2.0 * math.pi))

def encode(seq_block, w_up, w_down):
    tokens = seq_block.reshape(-1, seq_block.shape[-1])
    pre_act = jnp.dot(tokens, w_up.T, preferred_element_type=jnp.float32)
    hidden = jax.nn.gelu(pre_act, approximate=False).astype(jnp.bfloat16)
    summed = tokens.astype(jnp.float32) + jnp.dot(hidden, w_down, preferred_element_type=jnp.float32)
    row_mean = lax.optimization_barrier(jnp.mean(summed, -1, keepdims=True))
    centred = summed - row_mean
    inv_scale = lax.rsqrt(lax.optimization_barrier(jnp.mean(centred * centred, -1, keepdims=True)) + norm_eps)
    normed = centred * inv_scale
    return (tokens, pre_act, hidden, normed, inv_scale)

def backward(pre_act, normed, inv_scale, d_embed, length, w_down):
    grad_out = jnp.repeat(d_embed / length, length, axis=0)
    grad_resid = inv_scale * (grad_out - lax.optimization_barrier(jnp.mean(grad_out, -1, keepdims=True)) - normed * lax.optimization_barrier(jnp.mean(grad_out * normed, -1, keepdims=True)))
    grad_low = grad_resid.astype(jnp.bfloat16)
    grad_hidden = jnp.dot(grad_low, w_down.T, preferred_element_type=jnp.float32)
    grad_pre = (grad_hidden * gelu_slope(pre_act)).astype(jnp.bfloat16)
    return (grad_low, grad_pre)

def reference(q_hidden, p_hidden, w_up, w_down, pos_index, hard_index):
    block_rows = 8
    every_seq = jnp.concatenate([q_hidden.reshape(-1, LEN, D), p_hidden.reshape(-1, LEN, D)], 0)
    blocks = every_seq.reshape(-1, block_rows, LEN, D)

    def embed(seq_block):
        normed = encode(seq_block, w_up, w_down)[3]
        return lax.optimization_barrier(jnp.mean(normed.reshape(block_rows, LEN, D), 1)).astype(jnp.bfloat16)
    embedded = lax.map(embed, blocks).reshape(2, REPLICAS, GQ, D)
    query_embed = embedded[0]
    passage_embed = embedded[1]
    scores = jnp.einsum('rqd,rpd->rqp', query_embed.astype(jnp.float32), passage_embed.astype(jnp.float32))
    columns = jnp.arange(GP, dtype=jnp.int32)
    hard_mask = jnp.any(hard_index[..., None] == columns, axis=-2)
    logits = scores + HARD_BOOST * hard_mask.astype(jnp.float32)
    row_max = lax.optimization_barrier(jnp.max(logits, -1, keepdims=True))
    log_total = row_max + jnp.log(lax.optimization_barrier(jnp.sum(jnp.exp(logits - row_max), -1, keepdims=True)))
    target = pos_index[..., None] == columns
    picked = lax.optimization_barrier(jnp.sum(jnp.where(target, logits, 0.0), -1))
    loss_sum = jnp.sum(log_total[..., 0] - picked)
    weights = (jnp.exp(logits - log_total) - target.astype(jnp.float32)).astype(jnp.bfloat16)
    d_query = jnp.einsum('rqp,rpd->rqd', weights.astype(jnp.float32), passage_embed.astype(jnp.float32))
    d_passage = jnp.einsum('rqp,rqd->rpd', weights.astype(jnp.float32), query_embed.astype(jnp.float32))
    d_all = jnp.concatenate([d_query.reshape(-1, D), d_passage.reshape(-1, D)], 0).reshape(-1, block_rows, D)

    def accumulate(up_sum, items):
        seq_block, d_embed = items
        tokens, pre_act, hidden, normed, inv_scale = encode(seq_block, w_up, w_down)
        grad_low, grad_pre = backward(pre_act, normed, inv_scale, d_embed, LEN, w_down)
        up_sum = up_sum + jnp.dot(grad_pre.T, tokens, preferred_element_type=jnp.float32)
        return (up_sum, None)
    up_sum, unused = lax.scan(accumulate, jnp.zeros((FF, D), jnp.float32), (blocks, d_all))
    return (up_sum, loss_sum / (REPLICAS * GQ))
```

```python
import functools
import math

import jax
import jax.numpy as jnp
from jax import lax
from jax.experimental import pallas as pl
from jax.experimental.pallas import tpu as pltpu
from jax.sharding import Mesh
from jax.sharding import PartitionSpec as P

DP = ("y", "xl", "z", "c")
SWAP = ((0, 1), (1, 0))

norm_eps = 1e-06
HARD_BOOST = 1.5
SQRT_HALF = 1.0 / math.sqrt(2.0)
DENSITY = 1.0 / math.sqrt(2.0 * math.pi)
BF = jnp.bfloat16
F32 = jnp.float32
MIB = 1 << 20

WHOLE = pl.BlockSpec(memory_space=pltpu.VMEM)
SCALARS = pl.BlockSpec(memory_space=pltpu.SMEM)
ANYWHERE = pl.BlockSpec(memory_space=pl.ANY)

SPAN = 16


def rows_by_rows(left, right):
    return lax.dot_general(left, right, (((1,), (1,)), ((), ())), preferred_element_type=F32)


def call(body, outs, ins, scratch=(), vmem=24):
    return pl.pallas_call(
        body,
        out_shape=outs,
        in_specs=ins,
        out_specs=jax.tree.map(lambda _: WHOLE, outs),
        scratch_shapes=scratch,
        compiler_params=pltpu.CompilerParams(vmem_limit_bytes=vmem * MIB),
    )


def encode_body(chunk, pos, hard, q, p, wu_hbm, wd_hbm, message, normed_out, inv_out, wu, wd, sem_u, sem_d):
    hidden_units, features = wu.shape
    steps = hidden_units // chunk

    def copies(n):
        at = pl.ds(n * chunk, chunk)
        return (
            pltpu.make_async_copy(wu_hbm.at[at], wu.at[at], sem_u.at[n]),
            pltpu.make_async_copy(wd_hbm.at[at], wd.at[at], sem_d.at[n]),
        )

    for n in range(steps):
        for copy in copies(n):
            copy.start()
    tokens = jnp.concatenate([q[...], p[...]], 0)
    summed = tokens.astype(F32)
    for n in range(steps):
        at = pl.ds(n * chunk, chunk)
        up, down = copies(n)
        up.wait()
        pre_act = rows_by_rows(tokens, wu[at, :])
        hidden = (0.5 * pre_act * (1.0 + lax.erf(pre_act * SQRT_HALF))).astype(BF)
        down.wait()
        summed = summed + jnp.dot(hidden, wd[at, :], preferred_element_type=F32)
    row_mean = jnp.mean(summed, -1, keepdims=True)
    centred = summed - row_mean
    inv_scale = lax.rsqrt(jnp.mean(centred * centred, -1, keepdims=True) + norm_eps)
    normed = centred * inv_scale
    normed_out[...] = normed.astype(BF)
    inv_out[...] = jnp.transpose(jnp.broadcast_to(inv_scale, (inv_scale.shape[0], 128)))[:8]
    length = q.shape[0]
    rows = []
    for s in range(2):
        embed = jnp.mean(normed[s * length : (s + 1) * length], 0, keepdims=True)
        rows += [embed[:, k * 128 : (k + 1) * 128] for k in range(features // 128)]
    lane = lax.broadcasted_iota(jnp.int32, (1, 128), 1)
    index_row = jnp.where(lane == 0, pos[0, 0], jnp.where(lane == 1, hard[0, 0], hard[0, 1]))
    rows.append(index_row.astype(F32))
    rows.append(jnp.zeros((SPAN - len(rows), 128), F32))
    block = jnp.concatenate(rows, 0).astype(BF)
    message[...] = jnp.broadcast_to(block[None], message.shape)


def encode(pos, hard, q, p, w_up, w_down, peers):
    length, features = q.shape
    hidden_units = w_up.shape[0]
    chunk = 256
    steps = hidden_units // chunk
    return call(
        functools.partial(encode_body, chunk),
        (
            jax.ShapeDtypeStruct((peers, SPAN, 128), BF),
            jax.ShapeDtypeStruct((2 * length, features), BF),
            jax.ShapeDtypeStruct((8, 2 * length), F32),
        ),
        [SCALARS, SCALARS, WHOLE, WHOLE, ANYWHERE, ANYWHERE],
        [
            pltpu.VMEM((hidden_units, features), BF),
            pltpu.VMEM((hidden_units, features), BF),
            pltpu.SemaphoreType.DMA((steps,)),
            pltpu.SemaphoreType.DMA((steps,)),
        ],
    )(pos, hard, q, p, w_up, w_down)


def prepare_body(blocks, q, p, qs, ps, normed, normed_s, inv, inv_s, wu, wd, slope_out, along_out, wd_out, wu_mine):
    core = lax.axis_index("c")
    features = wu.shape[1]
    width = wu.shape[0] // blocks
    half = width // 2
    mine = lax.broadcasted_iota(jnp.int32, (half, width), 0)
    source = lax.broadcasted_iota(jnp.int32, (half, width), 1)
    run = half // 8
    skipped = sum((mine >= run * k).astype(jnp.int32) for k in range(1, 8))
    pick = (source == mine + run * (skipped + core)).astype(F32).astype(BF)
    for b in range(blocks):
        old, new = pl.ds(b * width, width), pl.ds(b * half, half)
        wu_mine[new, :] = jnp.dot(pick, wu[old, :], preferred_element_type=F32).astype(BF)
        wd_out[new, :] = jnp.dot(pick, wd[old, :], preferred_element_type=F32).astype(BF)
    tokens = jnp.concatenate([q[...], p[...], qs[...], ps[...]], 0)
    normed_all = jnp.concatenate([normed[...], normed_s[...]], 0)
    inv_all = jnp.concatenate([inv[0:1, :], inv_s[0:1, :]], 1)
    chunk = 256
    for n in range(wu_mine.shape[0] // chunk):
        at = pl.ds(n * chunk, chunk)
        pre_act = rows_by_rows(wu_mine[at, :], tokens)
        slope = 0.5 * (1.0 + lax.erf(pre_act * SQRT_HALF))
        slope = slope + pre_act * jnp.exp(-0.5 * pre_act * pre_act) * DENSITY
        scaled = slope * inv_all
        slope_out[at, :] = scaled.astype(BF)
        along_out[at, :] = (scaled * rows_by_rows(wd_out[at, :], normed_all)).astype(BF)


def prepare(blocks, q, p, qs, ps, normed, normed_s, inv, inv_s, w_up, w_down):
    hidden_units, features = w_up.shape
    half, count = hidden_units // 2, 4 * q.shape[0]
    return call(
        functools.partial(prepare_body, blocks),
        (
            jax.ShapeDtypeStruct((half, count), BF),
            jax.ShapeDtypeStruct((half, count), BF),
            jax.ShapeDtypeStruct((half, features), BF),
        ),
        [WHOLE] * 10,
        [pltpu.VMEM((half, features), BF)],
        vmem=28,
    )(q, p, qs, ps, normed, normed_s, inv, inv_s, w_up, w_down)


def gradient_body(gathered, slope, along, wd, q, p, qs, ps, normed, normed_s, terms, loss, wide, d_query, d_passage):
    core = lax.axis_index("c")
    place = (lax.axis_index("y") * 2 + lax.axis_index("xl")) * 8 + lax.axis_index("z")
    pool, features = d_query.shape
    cores_apart = pool // 2
    length = q.shape[0]
    wide[...] = gathered[...].astype(F32)
    parts = features // 128
    from_all = lambda k: wide[pl.ds(k, pool, stride=SPAN), :]
    queries = jnp.concatenate([from_all(k) for k in range(parts)], 1).astype(BF)
    passages = jnp.concatenate([from_all(parts + k) for k in range(parts)], 1).astype(BF)
    indices = from_all(2 * parts)
    lane = lax.broadcasted_iota(jnp.int32, (1, pool), 1)
    late = (lane >= cores_apart).astype(jnp.int32)
    column = (2 * (lane - cores_apart * late) + late).astype(F32)
    target = indices[:, 0:1] == column
    named = (indices[:, 1:2] == column) | (indices[:, 2:3] == column)
    logits = rows_by_rows(queries, passages) + jnp.where(named, HARD_BOOST, 0.0)
    row_max = jnp.max(logits, -1, keepdims=True)
    log_total = row_max + jnp.log(jnp.sum(jnp.exp(logits - row_max), -1, keepdims=True))
    picked = jnp.sum(jnp.where(target, logits, 0.0), -1, keepdims=True)
    loss[...] = jnp.broadcast_to(jnp.sum(log_total - picked, 0, keepdims=True), loss.shape)
    weights = (jnp.exp(logits - log_total) - jnp.where(target, 1.0, 0.0)).astype(BF)
    d_query[...] = jnp.dot(weights, passages, preferred_element_type=F32)
    d_passage[...] = lax.dot_general(
        weights, queries, (((0,), (0,)), ((), ())), preferred_element_type=F32
    )
    own = core * cores_apart + place
    sibling = (1 - core) * cores_apart + place
    grad = jnp.concatenate(
        [d[pl.ds(at, 1), :] for at in (own, sibling) for d in (d_query, d_passage)], 0
    ) * (1.0 / length)
    level = grad - jnp.mean(grad, -1, keepdims=True)
    both = jnp.concatenate([grad, level], 0)
    high = both.astype(BF)
    low = (both - high.astype(F32)).astype(BF)
    vectors = jnp.concatenate([high, low], 0)
    normed_all = jnp.concatenate([normed[...], normed_s[...]], 0)
    shares = rows_by_rows(vectors, normed_all)
    offsets = rows_by_rows(wd[...], vectors)
    pieces = []
    for s in range(4):
        at = slice(s * length, (s + 1) * length)
        share = (shares[s : s + 1, at] + shares[8 + s : 9 + s, at]) * (1.0 / features)
        offset = offsets[:, 4 + s : 5 + s] + offsets[:, 12 + s : 13 + s]
        piece = offset * slope[:, at].astype(F32) - share * along[:, at].astype(F32)
        pieces.append(piece.astype(BF))
    grad_pre = jnp.concatenate(pieces, 1)
    tokens = jnp.concatenate([q[...], p[...], qs[...], ps[...]], 0)
    terms[...] = jnp.dot(grad_pre, tokens, preferred_element_type=F32).astype(BF)


def gradient(gathered, slope, along, wd, q, p, qs, ps, normed, normed_s):
    half, features = wd.shape
    pool = gathered.shape[0] // SPAN
    return call(
        gradient_body,
        (jax.ShapeDtypeStruct((half, features), BF), jax.ShapeDtypeStruct((8, 128), F32)),
        [WHOLE] * 10,
        [
            pltpu.VMEM(gathered.shape, F32),
            pltpu.VMEM((pool, features), F32),
            pltpu.VMEM((pool, features), F32),
        ],
    )(gathered, slope, along, wd, q, p, qs, ps, normed, normed_s)


def add_near_body(own_rows, arrived, loss, out):
    senders, rows, features = arrived.shape
    total = arrived[0].astype(F32)
    for s in range(1, senders):
        total = total + arrived[s].astype(F32)
    groups = rows // own_rows
    spread = lax.broadcasted_iota(jnp.int32, (groups * 8, rows), 0)
    source = lax.broadcasted_iota(jnp.int32, (groups * 8, rows), 1)
    group = spread >> 3
    inner = spread & 7
    pick = ((inner < own_rows) & (source == own_rows * group + inner)).astype(F32).astype(BF)
    placed = jnp.dot(pick, total.astype(BF), preferred_element_type=F32)
    value = loss[0:1, 0:1]
    first = value.astype(BF).astype(F32)
    second = (value - first).astype(BF).astype(F32)
    third = value - first - second
    lane = lax.broadcasted_iota(jnp.int32, (1, features), 1)
    split = jnp.where(lane == 0, first, jnp.where(lane == 1, second, jnp.where(lane == 2, third, 0.0)))
    is_loss = (lax.broadcasted_iota(jnp.int32, (groups * 8, 1), 0) & 7) == own_rows
    out[...] = jnp.where(is_loss, split, placed).astype(BF)


def add_near(arrived, loss, own_rows):
    groups = arrived.shape[1] // own_rows
    return call(
        functools.partial(add_near_body, own_rows),
        jax.ShapeDtypeStruct((groups * 8, arrived.shape[2]), BF),
        [WHOLE] * 2,
    )(arrived, loss)


def add_far_body(count, arrived, rows, mean_loss):
    total = arrived[0].astype(F32)
    for s in range(1, arrived.shape[0]):
        total = total + arrived[s].astype(F32)
    own = rows.shape[0]
    rows[...] = total[:own]
    loss = arrived[0, own : own + 1, 0:128].astype(F32) + arrived[1, own : own + 1, 0:128].astype(F32)
    lane = lax.broadcasted_iota(jnp.int32, (1, 128), 1)
    mean_loss[...] = jnp.sum(jnp.where(lane < 3, loss, 0.0), -1, keepdims=True) * (1.0 / count)


def add_far(arrived, own_rows, count):
    return call(
        functools.partial(add_far_body, count),
        (
            jax.ShapeDtypeStruct((own_rows, arrived.shape[2]), F32),
            jax.ShapeDtypeStruct((1, 1), F32),
        ),
        [WHOLE],
    )(arrived)


def exchange(tiles, axes):
    return lax.all_to_all(tiles, axes, split_axis=0, concat_axis=0, tiled=True)


def shards(q_hidden, p_hidden, w_up, w_down, pos_index, hard_index):
    features = w_up.shape[1]
    q = q_hidden.reshape(-1, features)
    p = p_hidden.reshape(-1, features)
    near, far = ("y", "xl"), ("z", "xh")
    near_count = lax.axis_size(near)
    far_count = lax.axis_size(far)
    own_rows = w_up.shape[0] // (2 * near_count * far_count)
    peers = lax.axis_size(("y", "xl", "z"))
    qs, ps = (lax.ppermute(a, "c", SWAP) for a in (q, p))
    message, normed, inv = encode(pos_index, hard_index.reshape(1, -1), q, p, w_up, w_down, peers)
    gathered = exchange(message, ("y", "xl", "z"))
    normed_s, inv_s = (lax.ppermute(a, "c", SWAP) for a in (normed, inv))
    slope, along, wd = prepare(near_count, q, p, qs, ps, normed, normed_s, inv, inv_s, w_up, w_down)
    gathered = lax.all_gather(gathered, "c", axis=0, tiled=True)
    terms, loss = gradient(
        gathered.reshape(-1, 128), slope, along, wd, q, p, qs, ps, normed, normed_s
    )
    arrived = exchange(terms.reshape(near_count, -1, features), near)
    partial = add_near(arrived, loss, own_rows)
    arrived = exchange(partial.reshape(far_count, 8, features), far)
    count = lax.axis_size(DP) * lax.axis_size("xh")
    rows, mean_loss = add_far(arrived, own_rows, count)
    return rows, mean_loss.reshape(())


def solution(mesh):
    finer = Mesh(mesh.devices.reshape(4, 2, 8, 2, mesh.shape["rep"]), ("y", "xl", "z", "c", "xh"))
    return jax.shard_map(
        shards,
        mesh=finer,
        in_specs=(
            P("xh", DP, None, None),
            P("xh", DP, None, None),
            P(),
            P(),
            P("xh", DP),
            P("xh", DP, None),
        ),
        out_specs=(P((*DP, "xh"), None), P()),
        check_vma=False,
    )
```

```python
import functools
import math

import jax
import jax.numpy as jnp
from jax import lax
from jax.experimental import pallas as pl
from jax.experimental.pallas import tpu as pltpu
from jax.sharding import Mesh
from jax.sharding import PartitionSpec as P

DP = ("y", "xl", "z", "c")
SWAP = ((0, 1), (1, 0))

norm_eps = 1e-06
HARD_BOOST = 1.5
SQRT_HALF = 1.0 / math.sqrt(2.0)
DENSITY = 1.0 / math.sqrt(2.0 * math.pi)
BF = jnp.bfloat16
F32 = jnp.float32
MIB = 1 << 20

WHOLE = pl.BlockSpec(memory_space=pltpu.VMEM)
IN_HBM = pl.BlockSpec(memory_space=pltpu.HBM)

SPAN = 16


def rows_by_rows(left, right):
    return lax.dot_general(left, right, (((1,), (1,)), ((), ())), preferred_element_type=F32)


def start_all(copies):
    for copy in copies:
        copy.start()
    return copies


def wait_all(copies):
    for copy in copies:
        copy.wait()


def in_hbm(*arrays):
    return [pltpu.with_memory_space_constraint(a, pltpu.HBM) for a in arrays]


def call(body, outs, ins, scratch=(), vmem=24, place=None):
    return pl.pallas_call(
        body,
        out_shape=outs,
        in_specs=ins,
        out_specs=jax.tree.map(lambda _: WHOLE, outs) if place is None else place,
        scratch_shapes=scratch,
        compiler_params=pltpu.CompilerParams(vmem_limit_bytes=vmem * MIB),
    )


def encode_body(chunk, pos, hard_hbm, q, p, wu_hbm, wd_hbm, message, normed_out, inv_out, both, wu, wd, hard, sem, sem_u, sem_d):
    hidden_units, features = wu.shape
    length = q.shape[0]
    steps = hidden_units // chunk
    own = start_all(
        [
            pltpu.make_async_copy(q, both.at[pl.ds(0, length)], sem.at[0]),
            pltpu.make_async_copy(p, both.at[pl.ds(length, length)], sem.at[1]),
        ]
    )
    ups, downs = [], []
    for n in range(steps):
        at = pl.ds(n * chunk, chunk)
        ups.append(pltpu.make_async_copy(wu_hbm.at[at], wu.at[at], sem_u.at[n]))
        downs.append(pltpu.make_async_copy(wd_hbm.at[at], wd.at[at], sem_d.at[n]))
        start_all([ups[-1], downs[-1]])
    indices = start_all([pltpu.make_async_copy(hard_hbm, hard, sem.at[2])])
    wait_all(own)
    tokens = both[...]
    summed = tokens.astype(F32)
    for n in range(steps):
        at = pl.ds(n * chunk, chunk)
        ups[n].wait()
        pre_act = rows_by_rows(tokens, wu[at, :])
        hidden = (0.5 * pre_act * (1.0 + lax.erf(pre_act * SQRT_HALF))).astype(BF)
        downs[n].wait()
        summed = summed + jnp.dot(hidden, wd[at, :], preferred_element_type=F32)
    row_mean = jnp.mean(summed, -1, keepdims=True)
    centred = summed - row_mean
    inv_scale = lax.rsqrt(jnp.mean(centred * centred, -1, keepdims=True) + norm_eps)
    normed = centred * inv_scale
    normed_out[...] = normed.astype(BF)
    inv_out[...] = jnp.transpose(jnp.broadcast_to(inv_scale, (inv_scale.shape[0], 128)))[:8]
    wait_all(indices)
    rows = []
    for s in range(2):
        embed = jnp.mean(normed[s * length : (s + 1) * length], 0, keepdims=True)
        rows += [embed[:, k * 128 : (k + 1) * 128] for k in range(features // 128)]
    lane = lax.broadcasted_iota(jnp.int32, (1, 128), 1)
    index_row = jnp.where(lane == 0, pos[0, 0], jnp.where(lane == 1, hard[0, 0], hard[0, 1]))
    rows.append(index_row.astype(F32))
    rows.append(jnp.zeros((SPAN - len(rows), 128), F32))
    block = jnp.concatenate(rows, 0).astype(BF)
    message[...] = jnp.broadcast_to(block[None], message.shape)


def encode(pos, hard, q, p, w_up, w_down, peers):
    length, features = q.shape
    hidden_units = w_up.shape[0]
    chunk = 256
    steps = hidden_units // chunk
    return call(
        functools.partial(encode_body, chunk),
        (
            jax.ShapeDtypeStruct((peers, SPAN, 128), BF),
            jax.ShapeDtypeStruct((2 * length, features), BF),
            jax.ShapeDtypeStruct((8, 2 * length), F32),
        ),
        [pl.BlockSpec(memory_space=pltpu.SMEM)] + [IN_HBM] * 5,
        [
            pltpu.VMEM((2 * length, features), BF),
            pltpu.VMEM((hidden_units, features), BF),
            pltpu.VMEM((hidden_units, features), BF),
            pltpu.SMEM(hard.shape, jnp.int32),
            pltpu.SemaphoreType.DMA((3,)),
            pltpu.SemaphoreType.DMA((steps,)),
            pltpu.SemaphoreType.DMA((steps,)),
        ],
    )(pos, *in_hbm(hard, q, p, w_up, w_down))


def prepare_body(blocks, q, p, qs, ps, normed, normed_s, inv, inv_s, wu_hbm, wd_hbm, slope_hbm, along_hbm, wd_out, tokens_out, normed_out, wu, wd, wu_mine, wd_mine, tokens, normed_all, slope_all, along_all, sem_w, sem_t, sem_o, sem_n):
    core = lax.axis_index("c")
    width = wu.shape[0] // blocks
    half = width // 2
    length = q.shape[0]
    ups, downs = [], []
    for n in range(2):
        at = pl.ds(n * (wu.shape[0] // 2), wu.shape[0] // 2)
        ups.append(pltpu.make_async_copy(wu_hbm.at[at], wu.at[at], sem_w.at[n]))
        downs.append(pltpu.make_async_copy(wd_hbm.at[at], wd.at[at], sem_w.at[2 + n]))
    start_all(ups)
    moves = start_all(
        [
            pltpu.make_async_copy(part, tokens.at[pl.ds(k * length, length)], sem_t.at[k])
            for k, part in enumerate((q, p))
        ]
    )
    start_all(downs)
    tokens[2 * length : 3 * length] = qs[...]
    tokens[3 * length :] = ps[...]
    normed_all[: 2 * length] = normed[...]
    normed_all[2 * length :] = normed_s[...]
    mine = lax.broadcasted_iota(jnp.int32, (half, width), 0)
    source = lax.broadcasted_iota(jnp.int32, (half, width), 1)
    run = half // 8
    skipped = sum((mine >= run * k).astype(jnp.int32) for k in range(1, 8))
    pick = (source == mine + run * (skipped + core)).astype(F32).astype(BF)
    def pick_rows(copies, weights, to):
        for b in range(blocks):
            if b % (blocks // 2) == 0:
                copies[b // (blocks // 2)].wait()
            rows = jnp.dot(pick, weights[pl.ds(b * width, width), :], preferred_element_type=F32)
            to[pl.ds(b * half, half), :] = rows.astype(BF)

    pick_rows(ups, wu, wu_mine)
    wait_all(moves)
    leaving = start_all(
        [
            pltpu.make_async_copy(tokens, tokens_out, sem_o.at[0]),
            pltpu.make_async_copy(normed_all, normed_out, sem_o.at[1]),
        ]
    )
    pick_rows(downs, wd, wd_mine)
    leaving += start_all([pltpu.make_async_copy(wd_mine, wd_out, sem_o.at[2])])
    inv_all = jnp.concatenate([inv[0:1, :], inv_s[0:1, :]], 1)
    chunk = 256
    for n in range(wu_mine.shape[0] // chunk):
        at = pl.ds(n * chunk, chunk)
        pre_act = rows_by_rows(wu_mine[at, :], tokens[...])
        slope = 0.5 * (1.0 + lax.erf(pre_act * SQRT_HALF))
        slope = slope + pre_act * jnp.exp(-0.5 * pre_act * pre_act) * DENSITY
        scaled = slope * inv_all
        slope_all[at, :] = scaled.astype(BF)
        along_all[at, :] = (scaled * rows_by_rows(wd_mine[at, :], normed_all[...])).astype(BF)
        leaving += start_all(
            [
                pltpu.make_async_copy(slope_all.at[at], slope_hbm.at[at], sem_n.at[0, n]),
                pltpu.make_async_copy(along_all.at[at], along_hbm.at[at], sem_n.at[1, n]),
            ]
        )
    wait_all(leaving)


def prepare(blocks, q, p, qs, ps, normed, normed_s, inv, inv_s, w_up, w_down):
    hidden_units, features = w_up.shape
    half, count = hidden_units // 2, 4 * q.shape[0]
    shapes = ((half, count), (half, count), (half, features), (count, features), (count, features))
    return call(
        functools.partial(prepare_body, blocks),
        tuple(pltpu.HBM(shape, BF) for shape in shapes),
        [IN_HBM] * 2 + [WHOLE] * 6 + [IN_HBM] * 2,
        [
            pltpu.VMEM((hidden_units, features), BF),
            pltpu.VMEM((hidden_units, features), BF),
            pltpu.VMEM((half, features), BF),
            pltpu.VMEM((half, features), BF),
            pltpu.VMEM((count, features), BF),
            pltpu.VMEM((count, features), BF),
            pltpu.VMEM((half, count), BF),
            pltpu.VMEM((half, count), BF),
            pltpu.SemaphoreType.DMA((4,)),
            pltpu.SemaphoreType.DMA((2,)),
            pltpu.SemaphoreType.DMA((3,)),
            pltpu.SemaphoreType.DMA((2, half // 256)),
        ],
        vmem=28,
        place=(IN_HBM,) * 5,
    )(*in_hbm(q, p), qs, ps, normed, normed_s, inv, inv_s, *in_hbm(w_up, w_down))


def gradient_body(length, gathered, slope_hbm, along_hbm, wd_hbm, tokens_hbm, normed_hbm, terms, loss, wide, d_query, d_passage, slope, along, wd, tokens, normed_all, sem):
    arriving = {
        name: pltpu.make_async_copy(source, to, sem.at[k])
        for k, (name, source, to) in enumerate(
            (
                ("normed", normed_hbm, normed_all),
                ("wd", wd_hbm, wd),
                ("slope", slope_hbm, slope),
                ("along", along_hbm, along),
                ("tokens", tokens_hbm, tokens),
            )
        )
    }
    start_all(arriving.values())
    core = lax.axis_index("c")
    place = (lax.axis_index("y") * 2 + lax.axis_index("xl")) * 8 + lax.axis_index("z")
    pool, features = d_query.shape
    cores_apart = pool // 2
    wide[...] = gathered[...].astype(F32)
    parts = features // 128
    from_all = lambda k: wide[pl.ds(k, pool, stride=SPAN), :]
    queries = jnp.concatenate([from_all(k) for k in range(parts)], 1).astype(BF)
    passages = jnp.concatenate([from_all(parts + k) for k in range(parts)], 1).astype(BF)
    indices = from_all(2 * parts)
    lane = lax.broadcasted_iota(jnp.int32, (1, pool), 1)
    late = (lane >= cores_apart).astype(jnp.int32)
    column = (2 * (lane - cores_apart * late) + late).astype(F32)
    target = indices[:, 0:1] == column
    named = (indices[:, 1:2] == column) | (indices[:, 2:3] == column)
    logits = rows_by_rows(queries, passages) + jnp.where(named, HARD_BOOST, 0.0)
    row_max = jnp.max(logits, -1, keepdims=True)
    log_total = row_max + jnp.log(jnp.sum(jnp.exp(logits - row_max), -1, keepdims=True))
    picked = jnp.sum(jnp.where(target, logits, 0.0), -1, keepdims=True)
    loss[...] = jnp.broadcast_to(jnp.sum(log_total - picked, 0, keepdims=True), loss.shape)
    weights = (jnp.exp(logits - log_total) - jnp.where(target, 1.0, 0.0)).astype(BF)
    d_query[...] = jnp.dot(weights, passages, preferred_element_type=F32)
    d_passage[...] = lax.dot_general(
        weights, queries, (((0,), (0,)), ((), ())), preferred_element_type=F32
    )
    own = core * cores_apart + place
    sibling = (1 - core) * cores_apart + place
    grad = jnp.concatenate(
        [d[pl.ds(at, 1), :] for at in (own, sibling) for d in (d_query, d_passage)], 0
    ) * (1.0 / length)
    level = grad - jnp.mean(grad, -1, keepdims=True)
    both = jnp.concatenate([grad, level], 0)
    high = both.astype(BF)
    low = (both - high.astype(F32)).astype(BF)
    vectors = jnp.concatenate([high, low], 0)
    arriving["normed"].wait()
    shares = rows_by_rows(vectors, normed_all[...])
    arriving["wd"].wait()
    offsets = rows_by_rows(wd[...], vectors)
    arriving["slope"].wait()
    arriving["along"].wait()
    pieces = []
    for s in range(4):
        at = slice(s * length, (s + 1) * length)
        share = (shares[s : s + 1, at] + shares[8 + s : 9 + s, at]) * (1.0 / features)
        offset = offsets[:, 4 + s : 5 + s] + offsets[:, 12 + s : 13 + s]
        piece = offset * slope[:, at].astype(F32) - share * along[:, at].astype(F32)
        pieces.append(piece.astype(BF))
    grad_pre = jnp.concatenate(pieces, 1)
    arriving["tokens"].wait()
    terms[...] = jnp.dot(grad_pre, tokens[...], preferred_element_type=F32).astype(BF)


def gradient(length, gathered, slope, along, wd, tokens, normed):
    half, features = wd.shape
    pool = gathered.shape[0] // SPAN
    return call(
        functools.partial(gradient_body, length),
        (jax.ShapeDtypeStruct((half, features), BF), jax.ShapeDtypeStruct((8, 128), F32)),
        [WHOLE] + [IN_HBM] * 5,
        [
            pltpu.VMEM(gathered.shape, F32),
            pltpu.VMEM((pool, features), F32),
            pltpu.VMEM((pool, features), F32),
            *(pltpu.VMEM(a.shape, BF) for a in (slope, along, wd, tokens, normed)),
            pltpu.SemaphoreType.DMA((5,)),
        ],
    )(gathered, *in_hbm(slope, along, wd, tokens, normed))


def add_near_body(own_rows, arrived, loss, out):
    senders, rows, features = arrived.shape
    total = arrived[0].astype(F32)
    for s in range(1, senders):
        total = total + arrived[s].astype(F32)
    groups = rows // own_rows
    spread = lax.broadcasted_iota(jnp.int32, (groups * 8, rows), 0)
    source = lax.broadcasted_iota(jnp.int32, (groups * 8, rows), 1)
    group = spread >> 3
    inner = spread & 7
    pick = ((inner < own_rows) & (source == own_rows * group + inner)).astype(F32).astype(BF)
    placed = jnp.dot(pick, total.astype(BF), preferred_element_type=F32)
    value = loss[0:1, 0:1]
    first = value.astype(BF).astype(F32)
    second = (value - first).astype(BF).astype(F32)
    third = value - first - second
    lane = lax.broadcasted_iota(jnp.int32, (1, features), 1)
    split = jnp.where(lane == 0, first, jnp.where(lane == 1, second, jnp.where(lane == 2, third, 0.0)))
    is_loss = (lax.broadcasted_iota(jnp.int32, (groups * 8, 1), 0) & 7) == own_rows
    out[...] = jnp.where(is_loss, split, placed).astype(BF)


def add_near(arrived, loss, own_rows):
    groups = arrived.shape[1] // own_rows
    return call(
        functools.partial(add_near_body, own_rows),
        jax.ShapeDtypeStruct((groups * 8, arrived.shape[2]), BF),
        [WHOLE] * 2,
    )(arrived, loss)


def add_far_body(count, arrived, rows, mean_loss):
    total = arrived[0].astype(F32)
    for s in range(1, arrived.shape[0]):
        total = total + arrived[s].astype(F32)
    own = rows.shape[0]
    rows[...] = total[:own]
    loss = arrived[0, own : own + 1, 0:128].astype(F32) + arrived[1, own : own + 1, 0:128].astype(F32)
    lane = lax.broadcasted_iota(jnp.int32, (1, 128), 1)
    mean_loss[...] = jnp.sum(jnp.where(lane < 3, loss, 0.0), -1, keepdims=True) * (1.0 / count)


def add_far(arrived, own_rows, count):
    return call(
        functools.partial(add_far_body, count),
        (
            jax.ShapeDtypeStruct((own_rows, arrived.shape[2]), F32),
            jax.ShapeDtypeStruct((1, 1), F32),
        ),
        [WHOLE],
    )(arrived)


def exchange(tiles, axes):
    return lax.all_to_all(tiles, axes, split_axis=0, concat_axis=0, tiled=True)


def shards(q_hidden, p_hidden, w_up, w_down, pos_index, hard_index):
    features = w_up.shape[1]
    q = q_hidden.reshape(-1, features)
    p = p_hidden.reshape(-1, features)
    near, far = ("y", "xl"), ("z", "xh")
    near_count = lax.axis_size(near)
    far_count = lax.axis_size(far)
    own_rows = w_up.shape[0] // (2 * near_count * far_count)
    peers = lax.axis_size(("y", "xl", "z"))
    qs, ps = (lax.ppermute(a, "c", SWAP) for a in (q, p))
    message, normed, inv = encode(pos_index, hard_index.reshape(1, -1), q, p, w_up, w_down, peers)
    gathered = exchange(message, ("y", "xl", "z"))
    normed_s, inv_s = (lax.ppermute(a, "c", SWAP) for a in (normed, inv))
    slope, along, wd, tokens, normed_all = prepare(near_count, q, p, qs, ps, normed, normed_s, inv, inv_s, w_up, w_down)
    gathered = lax.all_gather(gathered, "c", axis=0, tiled=True)
    terms, loss = gradient(
        q.shape[0], gathered.reshape(-1, 128), slope, along, wd, tokens, normed_all
    )
    arrived = exchange(terms.reshape(near_count, -1, features), near)
    partial = add_near(arrived, loss, own_rows)
    arrived = exchange(partial.reshape(far_count, 8, features), far)
    count = lax.axis_size(DP) * lax.axis_size("xh")
    rows, mean_loss = add_far(arrived, own_rows, count)
    return rows, mean_loss.reshape(())


def solution(mesh):
    finer = Mesh(mesh.devices.reshape(4, 2, 8, 2, mesh.shape["rep"]), ("y", "xl", "z", "c", "xh"))
    return jax.shard_map(
        shards,
        mesh=finer,
        in_specs=(
            P("xh", DP, None, None),
            P("xh", DP, None, None),
            P(),
            P(),
            P("xh", DP),
            P("xh", DP, None),
        ),
        out_specs=(P((*DP, "xh"), None), P()),
        check_vma=False,
    )
```

```python
import functools
import math

import jax
import jax.numpy as jnp
from jax import lax
from jax.experimental import pallas as pl
from jax.experimental.pallas import tpu as pltpu
from jax.sharding import Mesh
from jax.sharding import PartitionSpec as P


DP = ("y", "xl", "z", "c")
SWAP = ((0, 1), (1, 0))

norm_eps = 1e-06
HARD_BOOST = 1.5
SQRT_HALF = 1.0 / math.sqrt(2.0)
DENSITY = 1.0 / math.sqrt(2.0 * math.pi)
BF = jnp.bfloat16
F32 = jnp.float32
MIB = 1 << 20

WHOLE = pl.BlockSpec(memory_space=pltpu.VMEM)
IN_HBM = pl.BlockSpec(memory_space=pltpu.HBM)

SPAN = 16
SPARE = 16


def rows_by_rows(left, right):
    return lax.dot_general(left, right, (((1,), (1,)), ((), ())), preferred_element_type=F32)


def start_all(copies):
    for copy in copies:
        copy.start()
    return copies


def wait_all(copies):
    for copy in copies:
        copy.wait()


def in_hbm(*arrays):
    return [pltpu.with_memory_space_constraint(a, pltpu.HBM) for a in arrays]


def call(body, outs, ins, scratch=(), vmem=24, place=None, flops=0):
    return pl.pallas_call(
        body,
        out_shape=outs,
        in_specs=ins,
        out_specs=jax.tree.map(lambda _: WHOLE, outs) if place is None else place,
        scratch_shapes=scratch,
        cost_estimate=pl.CostEstimate(flops=flops, transcendentals=0, bytes_accessed=0),
        compiler_params=pltpu.CompilerParams(vmem_limit_bytes=vmem * MIB),
    )


def split(value):
    first = value.astype(BF).astype(F32)
    second = (value - first).astype(BF).astype(F32)
    return first, second, value - first - second


def encode_body(chunk, pos, hard_hbm, q, p, wu_hbm, wd_hbm, message, shared, wu, wd, hard, sem, sem_u, sem_d):
    hidden_units, features = wu.shape
    length = q.shape[0]
    count = 2 * length
    steps = hidden_units // chunk
    own = start_all(
        [
            pltpu.make_async_copy(q, shared.at[pl.ds(0, length)], sem.at[0]),
            pltpu.make_async_copy(p, shared.at[pl.ds(length, length)], sem.at[1]),
        ]
    )
    ups, downs = [], []
    for n in range(steps):
        at = pl.ds(n * chunk, chunk)
        ups.append(pltpu.make_async_copy(wu_hbm.at[at], wu.at[at], sem_u.at[n]))
        downs.append(pltpu.make_async_copy(wd_hbm.at[at], wd.at[at], sem_d.at[n]))
        start_all([ups[-1], downs[-1]])
    indices = start_all([pltpu.make_async_copy(hard_hbm, hard, sem.at[2])])
    wait_all(own)
    tokens = shared[:count]
    summed = tokens.astype(F32)
    for n in range(steps):
        at = pl.ds(n * chunk, chunk)
        ups[n].wait()
        pre_act = rows_by_rows(tokens, wu[at, :])
        hidden = (0.5 * pre_act * (1.0 + lax.erf(pre_act * SQRT_HALF))).astype(BF)
        downs[n].wait()
        summed = summed + jnp.dot(hidden, wd[at, :], preferred_element_type=F32)
    row_mean = jnp.mean(summed, -1, keepdims=True)
    centred = summed - row_mean
    inv_scale = lax.rsqrt(jnp.mean(centred * centred, -1, keepdims=True) + norm_eps)
    normed = centred * inv_scale
    shared[count : 2 * count] = normed.astype(BF)
    inv_row = jnp.transpose(jnp.broadcast_to(inv_scale, (count, 128)))[:1]
    pieces = jnp.concatenate([*split(inv_row), jnp.zeros((SPARE - 3, count), F32)], 0)
    shared[2 * count :, :count] = pieces.astype(BF)
    shared[2 * count :, count:] = jnp.zeros((SPARE, features - count), BF)
    wait_all(indices)
    rows = []
    for s in range(2):
        embed = jnp.mean(normed[s * length : (s + 1) * length], 0, keepdims=True)
        rows += [embed[:, k * 128 : (k + 1) * 128] for k in range(features // 128)]
    lane = lax.broadcasted_iota(jnp.int32, (1, 128), 1)
    index_row = jnp.where(lane == 0, pos[0, 0], jnp.where(lane == 1, hard[0, 0], hard[0, 1]))
    rows.append(index_row.astype(F32))
    rows.append(jnp.zeros((SPAN - len(rows), 128), F32))
    block = jnp.concatenate(rows, 0).astype(BF)
    message[...] = jnp.broadcast_to(block[None], message.shape)


def encode(pos, hard, q, p, w_up, w_down, peers):
    length, features = q.shape
    hidden_units = w_up.shape[0]
    chunk = hidden_units // 2
    steps = hidden_units // chunk
    return call(
        functools.partial(encode_body, chunk),
        (
            jax.ShapeDtypeStruct((peers, SPAN, 128), BF),
            jax.ShapeDtypeStruct((4 * length + SPARE, features), BF),
        ),
        [pl.BlockSpec(memory_space=pltpu.SMEM)] + [IN_HBM] * 5,
        [
            pltpu.VMEM((hidden_units, features), BF),
            pltpu.VMEM((hidden_units, features), BF),
            pltpu.SMEM(hard.shape, jnp.int32),
            pltpu.SemaphoreType.DMA((3,)),
            pltpu.SemaphoreType.DMA((steps,)),
            pltpu.SemaphoreType.DMA((steps,)),
        ],
    )(pos, *in_hbm(hard, q, p, w_up, w_down))


def prepare_body(blocks, shared, shared_s, wu_hbm, wd_hbm, slope_hbm, tokens_hbm, wd_out, along, normed_all, wu, wd, wu_mine, wd_mine, tokens, slope_all, sem_u, sem_d, sem_o):
    core = lax.axis_index("c")
    width = wu.shape[0] // blocks
    half = width // 2
    count = tokens.shape[0] // 2
    ups, downs = [], []
    parts = 2
    for n in range(parts):
        at = pl.ds(n * (wu.shape[0] // parts), wu.shape[0] // parts)
        ups.append(pltpu.make_async_copy(wu_hbm.at[at], wu.at[at], sem_u.at[n]))
        downs.append(pltpu.make_async_copy(wd_hbm.at[at], wd.at[at], sem_d.at[n]))
    start_all(ups)
    tokens[:count] = shared[:count]
    tokens[count:] = shared_s[:count]
    normed_all[:count] = shared[count : 2 * count]
    normed_all[count:] = shared_s[count : 2 * count]
    mine = lax.broadcasted_iota(jnp.int32, (half, width), 0)
    source = lax.broadcasted_iota(jnp.int32, (half, width), 1)
    run = half // 8
    skipped = sum((mine >= run * k).astype(jnp.int32) for k in range(1, 8))
    pick = (source == mine + run * (skipped + core)).astype(F32).astype(BF)
    def pick_rows(copies, weights, to, then=()):
        for b in range(blocks):
            if b % (blocks // parts) == 0:
                copies[b // (blocks // parts)].wait()
                start_all(then[b // (blocks // parts) :][:1])
            rows = jnp.dot(pick, weights[pl.ds(b * width, width), :], preferred_element_type=F32)
            to[pl.ds(b * half, half), :] = rows.astype(BF)

    leaving = start_all([pltpu.make_async_copy(tokens, tokens_hbm, sem_o.at[0])])
    pick_rows(ups, wu, wu_mine, downs)
    pre_act = rows_by_rows(wu_mine[...], tokens[...])
    pick_rows(downs, wd, wd_mine)
    leaving += start_all([pltpu.make_async_copy(wd_mine, wd_out, sem_o.at[2])])
    inv_all = jnp.concatenate(
        [jnp.sum(a[2 * count :, :count].astype(F32), 0, keepdims=True) for a in (shared, shared_s)], 1
    )
    slope = 0.5 * (1.0 + lax.erf(pre_act * SQRT_HALF))
    slope = slope + pre_act * jnp.exp(-0.5 * pre_act * pre_act) * DENSITY
    scaled = slope * inv_all
    slope_all[...] = scaled.astype(BF)
    leaving += start_all([pltpu.make_async_copy(slope_all, slope_hbm, sem_o.at[1])])
    along[...] = (scaled * rows_by_rows(wd_mine[...], normed_all[...])).astype(BF)
    wait_all(leaving)


def prepare(blocks, shared, shared_s, w_up, w_down):
    hidden_units, features = w_up.shape
    half, count = hidden_units // 2, (shared.shape[0] - SPARE)
    shapes = ((half, count), (count, features), (half, features))
    return call(
        functools.partial(prepare_body, blocks),
        (
            *(pltpu.HBM(shape, BF) for shape in shapes),
            jax.ShapeDtypeStruct((half, count), BF),
            jax.ShapeDtypeStruct((count, features), BF),
        ),
        [WHOLE] * 2 + [IN_HBM] * 2,
        [
            pltpu.VMEM((hidden_units, features), BF),
            pltpu.VMEM((hidden_units, features), BF),
            pltpu.VMEM((half, features), BF),
            pltpu.VMEM((half, features), BF),
            pltpu.VMEM((count, features), BF),
            pltpu.VMEM((half, count), BF),
            pltpu.SemaphoreType.DMA((2,)),
            pltpu.SemaphoreType.DMA((2,)),
            pltpu.SemaphoreType.DMA((3,)),
        ],
        vmem=28,
        place=(IN_HBM,) * 3 + (WHOLE,) * 2,
        flops=8 * half * count * features,
    )(shared, shared_s, *in_hbm(w_up, w_down))


def gradient_body(length, gathered, along, normed_all, wd_hbm, slope_hbm, tokens_hbm, terms, loss, wide, d_query, d_passage, wd, slope, tokens, sem):
    arriving = start_all(
        [
            pltpu.make_async_copy(source, to, sem.at[k])
            for k, (source, to) in enumerate(
                ((wd_hbm, wd), (slope_hbm, slope), (tokens_hbm, tokens))
            )
        ]
    )
    core = lax.axis_index("c")
    place = (lax.axis_index("y") * 2 + lax.axis_index("xl")) * 8 + lax.axis_index("z")
    pool, features = d_query.shape
    cores_apart = pool // 2
    wide[...] = gathered[...].astype(F32)
    parts = features // 128
    from_all = lambda k: wide[pl.ds(k, pool, stride=SPAN), :]
    queries = jnp.concatenate([from_all(k) for k in range(parts)], 1).astype(BF)
    passages = jnp.concatenate([from_all(parts + k) for k in range(parts)], 1).astype(BF)
    indices = from_all(2 * parts)
    lane = lax.broadcasted_iota(jnp.int32, (1, pool), 1)
    late = (lane >= cores_apart).astype(jnp.int32)
    column = (2 * (lane - cores_apart * late) + late).astype(F32)
    target = indices[:, 0:1] == column
    named = (indices[:, 1:2] == column) | (indices[:, 2:3] == column)
    logits = rows_by_rows(queries, passages) + jnp.where(named, HARD_BOOST, 0.0)
    row_max = jnp.max(logits, -1, keepdims=True)
    log_total = row_max + jnp.log(jnp.sum(jnp.exp(logits - row_max), -1, keepdims=True))
    picked = jnp.sum(jnp.where(target, logits, 0.0), -1, keepdims=True)
    loss[...] = jnp.broadcast_to(jnp.sum(log_total - picked, 0, keepdims=True), loss.shape)
    weights = (jnp.exp(logits - log_total) - jnp.where(target, 1.0, 0.0)).astype(BF)
    d_query[...] = jnp.dot(weights, passages, preferred_element_type=F32)
    d_passage[...] = lax.dot_general(
        weights, queries, (((0,), (0,)), ((), ())), preferred_element_type=F32
    )
    own = core * cores_apart + place
    sibling = (1 - core) * cores_apart + place
    grad = jnp.concatenate(
        [d[pl.ds(at, 1), :] for at in (own, sibling) for d in (d_query, d_passage)], 0
    ) * (1.0 / length)
    level = grad - jnp.mean(grad, -1, keepdims=True)
    both = jnp.concatenate([grad, level], 0)
    high = both.astype(BF)
    low = (both - high.astype(F32)).astype(BF)
    vectors = jnp.concatenate([high, low], 0)
    shares = rows_by_rows(vectors, normed_all[...])
    arriving[0].wait()
    offsets = rows_by_rows(wd[...], vectors)
    arriving[1].wait()
    pieces = []
    for s in range(4):
        at = slice(s * length, (s + 1) * length)
        share = (shares[s : s + 1, at] + shares[8 + s : 9 + s, at]) * (1.0 / features)
        offset = offsets[:, 4 + s : 5 + s] + offsets[:, 12 + s : 13 + s]
        piece = offset * slope[:, at].astype(F32) - share * along[:, at].astype(F32)
        pieces.append(piece.astype(BF))
    grad_pre = jnp.concatenate(pieces, 1)
    arriving[2].wait()
    terms[...] = jnp.dot(grad_pre, tokens[...], preferred_element_type=F32).astype(BF)


def gradient(length, gathered, along, normed, wd, slope, tokens):
    half, features = wd.shape
    pool = gathered.shape[0] // SPAN
    return call(
        functools.partial(gradient_body, length),
        (jax.ShapeDtypeStruct((half, features), BF), jax.ShapeDtypeStruct((8, 128), F32)),
        [WHOLE] * 3 + [IN_HBM] * 3,
        [
            pltpu.VMEM(gathered.shape, F32),
            pltpu.VMEM((pool, features), F32),
            pltpu.VMEM((pool, features), F32),
            *(pltpu.VMEM(a.shape, BF) for a in (wd, slope, tokens)),
            pltpu.SemaphoreType.DMA((3,)),
        ],
    )(gathered, along, normed, *in_hbm(wd, slope, tokens))


def add_near_body(own_rows, arrived, loss, out):
    senders, rows, features = arrived.shape
    total = arrived[0].astype(F32)
    for s in range(1, senders):
        total = total + arrived[s].astype(F32)
    groups = rows // own_rows
    spread = lax.broadcasted_iota(jnp.int32, (groups * 8, rows), 0)
    source = lax.broadcasted_iota(jnp.int32, (groups * 8, rows), 1)
    group = spread >> 3
    inner = spread & 7
    pick = ((inner < own_rows) & (source == own_rows * group + inner)).astype(F32).astype(BF)
    placed = jnp.dot(pick, total.astype(BF), preferred_element_type=F32)
    first, second, third = split(loss[0:1, 0:1])
    lane = lax.broadcasted_iota(jnp.int32, (1, features), 1)
    pieces = jnp.where(lane == 0, first, jnp.where(lane == 1, second, jnp.where(lane == 2, third, 0.0)))
    is_loss = (lax.broadcasted_iota(jnp.int32, (groups * 8, 1), 0) & 7) == own_rows
    out[...] = jnp.where(is_loss, pieces, placed).astype(BF)


def add_near(arrived, loss, own_rows):
    groups = arrived.shape[1] // own_rows
    return call(
        functools.partial(add_near_body, own_rows),
        jax.ShapeDtypeStruct((groups * 8, arrived.shape[2]), BF),
        [WHOLE] * 2,
    )(arrived, loss)


def add_far_body(count, arrived, rows, mean_loss):
    total = arrived[0].astype(F32)
    for s in range(1, arrived.shape[0]):
        total = total + arrived[s].astype(F32)
    own = rows.shape[0]
    rows[...] = total[:own]
    loss = arrived[0, own : own + 1, 0:128].astype(F32) + arrived[1, own : own + 1, 0:128].astype(F32)
    lane = lax.broadcasted_iota(jnp.int32, (1, 128), 1)
    mean_loss[...] = jnp.sum(jnp.where(lane < 3, loss, 0.0), -1, keepdims=True) * (1.0 / count)


def add_far(arrived, own_rows, count):
    return call(
        functools.partial(add_far_body, count),
        (
            jax.ShapeDtypeStruct((own_rows, arrived.shape[2]), F32),
            jax.ShapeDtypeStruct((1, 1), F32),
        ),
        [WHOLE],
    )(arrived)


def exchange(tiles, axes):
    return lax.all_to_all(tiles, axes, split_axis=0, concat_axis=0, tiled=True)


def step(q_hidden, p_hidden, w_up, w_down, pos_index, hard_index):
    features = w_up.shape[1]
    q = q_hidden.reshape(-1, features)
    p = p_hidden.reshape(-1, features)
    near, far = ("y", "xl"), ("z", "xh")
    near_count = lax.axis_size(near)
    far_count = lax.axis_size(far)
    own_rows = w_up.shape[0] // (2 * near_count * far_count)
    peers = lax.axis_size(("y", "xl", "z"))
    message, shared = encode(pos_index, hard_index.reshape(1, -1), q, p, w_up, w_down, peers)
    gathered = exchange(message, ("y", "xl", "z"))
    shared_s = lax.ppermute(shared, "c", SWAP)
    slope, tokens, wd, along, normed = prepare(near_count, shared, shared_s, w_up, w_down)
    gathered = lax.all_gather(gathered, "c", axis=0, tiled=True)
    terms, loss = gradient(
        q.shape[0], gathered.reshape(-1, 128), along, normed, wd, slope, tokens
    )
    arrived = exchange(terms.reshape(near_count, -1, features), near)
    partial = add_near(arrived, loss, own_rows)
    arrived = exchange(partial.reshape(far_count, 8, features), far)
    count = lax.axis_size(DP) * lax.axis_size("xh")
    rows, mean_loss = add_far(arrived, own_rows, count)
    return rows, mean_loss.reshape(())


def solution(mesh):
    finer = Mesh(mesh.devices.reshape(4, 2, 8, 2, mesh.shape["rep"]), ("y", "xl", "z", "c", "xh"))
    return jax.shard_map(
        step,
        mesh=finer,
        in_specs=(
            P("xh", DP, None, None),
            P("xh", DP, None, None),
            P(),
            P(),
            P("xh", DP),
            P("xh", DP, None),
        ),
        out_specs=(P((*DP, "xh"), None), P()),
        check_vma=False,
    )
```

```python
import functools
import math

import jax
import jax.numpy as jnp
from jax import lax
from jax.experimental import pallas as pl
from jax.experimental.pallas import tpu as pltpu
from jax.sharding import Mesh
from jax.sharding import PartitionSpec as P


DP = ("y", "xl", "z", "c")
SWAP = ((0, 1), (1, 0))

norm_eps = 1e-06
HARD_BOOST = 1.5
SQRT_HALF = 1.0 / math.sqrt(2.0)
DENSITY = 1.0 / math.sqrt(2.0 * math.pi)
BF = jnp.bfloat16
F32 = jnp.float32
MIB = 1 << 20

WHOLE = pl.BlockSpec(memory_space=pltpu.VMEM)
IN_HBM = pl.BlockSpec(memory_space=pltpu.HBM)

SPAN = 16
SPARE = 16


def rows_by_rows(left, right):
    return lax.dot_general(left, right, (((1,), (1,)), ((), ())), preferred_element_type=F32)


def start_all(copies):
    for copy in copies:
        copy.start()
    return copies


def wait_all(copies):
    for copy in copies:
        copy.wait()


def in_hbm(*arrays):
    return [pltpu.with_memory_space_constraint(a, pltpu.HBM) for a in arrays]


def call(body, outs, ins, scratch=(), vmem=24, place=None, flops=0):
    return pl.pallas_call(
        body,
        out_shape=outs,
        in_specs=ins,
        out_specs=jax.tree.map(lambda _: WHOLE, outs) if place is None else place,
        scratch_shapes=scratch,
        cost_estimate=pl.CostEstimate(flops=flops, transcendentals=0, bytes_accessed=0),
        compiler_params=pltpu.CompilerParams(vmem_limit_bytes=vmem * MIB),
    )


def split(value):
    first = value.astype(BF).astype(F32)
    second = (value - first).astype(BF).astype(F32)
    return first, second, value - first - second


def encode_body(chunk, *refs):
    sends = len(refs) == 14
    if sends:
        pos, hard_hbm, q, p, wu_hbm, wd_hbm, message, shared, wu, wd, sem, sem_u, sem_d, hard = refs
    else:
        q, p, wu_hbm, wd_hbm, shared, wu, wd, sem, sem_u, sem_d = refs
    hidden_units, features = wu.shape
    length = q.shape[0]
    count = 2 * length
    steps = hidden_units // chunk
    own = start_all(
        [
            pltpu.make_async_copy(q, shared.at[pl.ds(0, length)], sem.at[0]),
            pltpu.make_async_copy(p, shared.at[pl.ds(length, length)], sem.at[1]),
        ]
    )
    ups, downs = [], []
    for n in range(steps):
        at = pl.ds(n * chunk, chunk)
        ups.append(pltpu.make_async_copy(wu_hbm.at[at], wu.at[at], sem_u.at[n]))
        downs.append(pltpu.make_async_copy(wd_hbm.at[at], wd.at[at], sem_d.at[n]))
        start_all([ups[-1], downs[-1]])
    indices = start_all([pltpu.make_async_copy(hard_hbm, hard, sem.at[2])] if sends else [])
    wait_all(own)
    tokens = shared[:count]
    summed = tokens.astype(F32)
    for n in range(steps):
        at = pl.ds(n * chunk, chunk)
        ups[n].wait()
        pre_act = rows_by_rows(tokens, wu[at, :])
        hidden = (0.5 * pre_act * (1.0 + lax.erf(pre_act * SQRT_HALF))).astype(BF)
        downs[n].wait()
        summed = summed + jnp.dot(hidden, wd[at, :], preferred_element_type=F32)
    row_mean = jnp.mean(summed, -1, keepdims=True)
    centred = summed - row_mean
    inv_scale = lax.rsqrt(jnp.mean(centred * centred, -1, keepdims=True) + norm_eps)
    normed = centred * inv_scale
    shared[count : 2 * count] = normed.astype(BF)
    inv_row = jnp.transpose(jnp.broadcast_to(inv_scale, (count, 128)))[:1]
    pieces = jnp.concatenate([*split(inv_row), jnp.zeros((SPARE - 3, count), F32)], 0)
    shared[2 * count :, :count] = pieces.astype(BF)
    shared[2 * count :, count:] = jnp.zeros((SPARE, features - count), BF)
    if not sends:
        return
    wait_all(indices)
    rows = []
    for s in range(2):
        embed = jnp.mean(normed[s * length : (s + 1) * length], 0, keepdims=True)
        rows += [embed[:, k * 128 : (k + 1) * 128] for k in range(features // 128)]
    lane = lax.broadcasted_iota(jnp.int32, (1, 128), 1)
    index_row = jnp.where(lane == 0, pos[0, 0], jnp.where(lane == 1, hard[0, 0], hard[0, 1]))
    rows.append(index_row.astype(F32))
    rows.append(jnp.zeros((SPAN - len(rows), 128), F32))
    block = jnp.concatenate(rows, 0).astype(BF)
    message[...] = jnp.broadcast_to(block[None], message.shape)


def encode(q, p, w_up, w_down, indices=None, peers=0):
    length, features = q.shape
    hidden_units = w_up.shape[0]
    chunk = hidden_units // 2
    steps = hidden_units // chunk
    shared = jax.ShapeDtypeStruct((4 * length + SPARE, features), BF)
    scratch = [
        pltpu.VMEM((hidden_units, features), BF),
        pltpu.VMEM((hidden_units, features), BF),
        pltpu.SemaphoreType.DMA((3,)),
        pltpu.SemaphoreType.DMA((steps,)),
        pltpu.SemaphoreType.DMA((steps,)),
    ]
    body = functools.partial(encode_body, chunk)
    flops = 8 * length * features * hidden_units
    if indices is None:
        places = [WHOLE] * 2 + [IN_HBM] * 2
        return call(body, shared, places, scratch, flops=flops)(q, p, *in_hbm(w_up, w_down))
    pos, hard = indices
    return call(
        body,
        (jax.ShapeDtypeStruct((peers, SPAN, 128), BF), shared),
        [pl.BlockSpec(memory_space=pltpu.SMEM)] + [IN_HBM] * 5,
        [*scratch, pltpu.SMEM(hard.shape, jnp.int32)],
        flops=flops,
    )(pos, *in_hbm(hard, q, p, w_up, w_down))


def slopes(count, pair, wu_mine, wd_mine, tokens, normed_all, slope_all, along, slope_hbm, sem, between=None):
    pre_act = rows_by_rows(wu_mine[...], tokens[...])
    if between is not None:
        between()
    inv_all = jnp.concatenate(
        [jnp.sum(a[2 * count :, :count].astype(F32), 0, keepdims=True) for a in pair], 1
    )
    slope = 0.5 * (1.0 + lax.erf(pre_act * SQRT_HALF))
    slope = slope + pre_act * jnp.exp(-0.5 * pre_act * pre_act) * DENSITY
    scaled = slope * inv_all
    slope_all[...] = scaled.astype(BF)
    leaving = start_all([pltpu.make_async_copy(slope_all, slope_hbm, sem)])
    along[...] = (scaled * rows_by_rows(wd_mine[...], normed_all[...])).astype(BF)
    wait_all(leaving)


def lay_out(count, pair, tokens, normed_all, tokens_hbm, normed_hbm, sem):
    for k, shared in enumerate(pair):
        tokens[k * count : (k + 1) * count] = shared[:count]
        normed_all[k * count : (k + 1) * count] = shared[count : 2 * count]
    return start_all(
        [
            pltpu.make_async_copy(tokens, tokens_hbm, sem.at[0]),
            pltpu.make_async_copy(normed_all, normed_hbm, sem.at[1]),
        ]
    )


def prepare_near_body(width, shared, shared_s, wu_hbm, wd_hbm, slope_hbm, tokens_hbm, normed_hbm, wd_out, along, wu_mine, wd_mine, wu, wd, tokens, normed_all, slope_all, sem_u, sem_d, sem_o):
    core = lax.axis_index("c")
    side = lax.axis_index("xl")
    half = width // 2
    blocks = wu.shape[0] // width
    count = tokens.shape[0] // 2

    def copies(weights_hbm, weights, sem):
        return [
            pltpu.make_async_copy(
                weights_hbm.at[pl.ds(pl.multiple_of((2 * b + side) * width, width), width)],
                weights.at[pl.ds(b * width, width)],
                sem.at[b],
            )
            for b in range(blocks)
        ]

    ups = start_all(copies(wu_hbm, wu, sem_u))
    downs = start_all(copies(wd_hbm, wd, sem_d))
    leaving = lay_out(count, (shared, shared_s), tokens, normed_all, tokens_hbm, normed_hbm, sem_o)
    mine = lax.broadcasted_iota(jnp.int32, (half, width), 0)
    source = lax.broadcasted_iota(jnp.int32, (half, width), 1)
    run = half // 8
    skipped = sum((mine >= run * k).astype(jnp.int32) for k in range(1, 8))
    pick = (source == mine + run * (skipped + core)).astype(F32).astype(BF)

    def pick_rows(weights, to):
        for b in range(blocks):
            rows = jnp.dot(pick, weights[pl.ds(b * width, width), :], preferred_element_type=F32)
            to[pl.ds(b * half, half), :] = rows.astype(BF)

    wait_all(ups)
    pick_rows(wu, wu_mine)

    def pick_downs():
        wait_all(downs)
        pick_rows(wd, wd_mine)
        leaving.extend(start_all([pltpu.make_async_copy(wd_mine, wd_out, sem_o.at[2])]))

    slopes(count, (shared, shared_s), wu_mine, wd_mine, tokens, normed_all, slope_all, along, slope_hbm, sem_o.at[3], pick_downs)
    wait_all(leaving)


def prepare_near(blocks, shared, shared_s, w_up, w_down):
    hidden_units, features = w_up.shape
    quarter, count = hidden_units // 4, shared.shape[0] - SPARE
    shapes = ((quarter, count), (count, features), (count, features), (quarter, features))
    mine = jax.ShapeDtypeStruct((quarter, features), BF)
    return call(
        functools.partial(prepare_near_body, hidden_units // (2 * blocks)),
        (*(pltpu.HBM(shape, BF) for shape in shapes), jax.ShapeDtypeStruct((quarter, count), BF), mine, mine),
        [WHOLE] * 2 + [IN_HBM] * 2,
        [
            pltpu.VMEM((2 * quarter, features), BF),
            pltpu.VMEM((2 * quarter, features), BF),
            pltpu.VMEM((count, features), BF),
            pltpu.VMEM((count, features), BF),
            pltpu.VMEM((quarter, count), BF),
            pltpu.SemaphoreType.DMA((blocks,)),
            pltpu.SemaphoreType.DMA((blocks,)),
            pltpu.SemaphoreType.DMA((4,)),
        ],
        place=(IN_HBM,) * 4 + (WHOLE,) * 3,
        flops=8 * quarter * count * features,
    )(shared, shared_s, *in_hbm(w_up, w_down))


def prepare_far_body(shared, shared_s, wu_mine, wd_mine, slope_hbm, tokens_hbm, normed_hbm, along, tokens, normed_all, slope_all, sem_o):
    count = tokens.shape[0] // 2
    pair = (shared, shared_s)
    leaving = lay_out(count, pair, tokens, normed_all, tokens_hbm, normed_hbm, sem_o)
    slopes(count, pair, wu_mine, wd_mine, tokens, normed_all, slope_all, along, slope_hbm, sem_o.at[2])
    wait_all(leaving)


def prepare_far(shared, shared_s, wu_mine, wd_mine):
    quarter, features = wu_mine.shape
    count = shared.shape[0] - SPARE
    shapes = ((quarter, count), (count, features), (count, features))
    return call(
        prepare_far_body,
        (*(pltpu.HBM(shape, BF) for shape in shapes), jax.ShapeDtypeStruct((quarter, count), BF)),
        [WHOLE] * 4,
        [
            pltpu.VMEM((count, features), BF),
            pltpu.VMEM((count, features), BF),
            pltpu.VMEM((quarter, count), BF),
            pltpu.SemaphoreType.DMA((3,)),
        ],
        place=(IN_HBM,) * 3 + (WHOLE,),
        flops=8 * quarter * count * features,
    )(shared, shared_s, wu_mine, wd_mine)


def gradient_body(length, gathered, along, along_f, wd_hbm, slope_hbm, slope_f_hbm, tokens_hbm, tokens_f_hbm, normed_hbm, normed_f_hbm, terms, loss, wide, d_query, d_passage, wd, slope, tokens, normed_all, sem):
    half = 4 * length
    low, high = pl.ds(0, half), pl.ds(half, half)
    order = (
        (normed_hbm, normed_all.at[low]),
        (normed_f_hbm, normed_all.at[high]),
        (wd_hbm, wd),
        (slope_hbm, slope.at[0]),
        (slope_f_hbm, slope.at[1]),
        (tokens_hbm, tokens.at[low]),
        (tokens_f_hbm, tokens.at[high]),
    )
    arriving = start_all([pltpu.make_async_copy(*pair, sem.at[k]) for k, pair in enumerate(order)])
    core, side = lax.axis_index("c"), lax.axis_index("xl")
    row, layer = lax.axis_index("y"), lax.axis_index("z")
    pool, features = d_query.shape
    cores_apart = pool // 2
    wide[...] = gathered[...].astype(F32)
    parts = features // 128
    from_all = lambda k: wide[pl.ds(k, pool, stride=SPAN), :]
    queries = jnp.concatenate([from_all(k) for k in range(parts)], 1).astype(BF)
    passages = jnp.concatenate([from_all(parts + k) for k in range(parts)], 1).astype(BF)
    indices = from_all(2 * parts)
    lane = lax.broadcasted_iota(jnp.int32, (1, pool), 1)
    late = (lane >= cores_apart).astype(jnp.int32)
    column = (2 * (lane - cores_apart * late) + late).astype(F32)
    target = indices[:, 0:1] == column
    named = (indices[:, 1:2] == column) | (indices[:, 2:3] == column)
    logits = rows_by_rows(queries, passages) + jnp.where(named, HARD_BOOST, 0.0)
    row_max = jnp.max(logits, -1, keepdims=True)
    log_total = row_max + jnp.log(jnp.sum(jnp.exp(logits - row_max), -1, keepdims=True))
    picked = jnp.sum(jnp.where(target, logits, 0.0), -1, keepdims=True)
    loss[...] = jnp.broadcast_to(jnp.sum(log_total - picked, 0, keepdims=True), loss.shape)
    weights = (jnp.exp(logits - log_total) - jnp.where(target, 1.0, 0.0)).astype(BF)
    d_query[...] = jnp.dot(weights, passages, preferred_element_type=F32)
    d_passage[...] = lax.dot_general(
        weights, queries, (((0,), (0,)), ((), ())), preferred_element_type=F32
    )
    places = [
        c * cores_apart + (row * 2 + x) * 8 + layer for x in (side, 1 - side) for c in (core, 1 - core)
    ]
    grad = jnp.concatenate(
        [d[pl.ds(at, 1), :] for at in places for d in (d_query, d_passage)], 0
    ) * (1.0 / length)
    count = 2 * len(places)
    level = grad - jnp.mean(grad, -1, keepdims=True)
    both = jnp.concatenate([grad, level], 0)
    first = both.astype(BF)
    rest = (both - first.astype(F32)).astype(BF)
    vectors = jnp.concatenate([first, rest], 0)
    wait_all(arriving[:2])
    shares = rows_by_rows(vectors, normed_all[...])
    arriving[2].wait()
    offsets = rows_by_rows(wd[...], vectors)
    wait_all(arriving[3:5])
    pieces = []
    for s in range(count):
        at = slice(s * length, (s + 1) * length)
        inside = slice((s % 4) * length, (s % 4 + 1) * length)
        share = (shares[s : s + 1, at] + shares[2 * count + s : 2 * count + s + 1, at]) * (1.0 / features)
        u, v = count + s, 3 * count + s
        offset = offsets[:, u : u + 1] + offsets[:, v : v + 1]
        toward = (along, along_f)[s // 4][:, inside].astype(F32)
        pieces.append((offset * slope[s // 4, :, inside].astype(F32) - share * toward).astype(BF))
    grad_pre = jnp.concatenate(pieces, 1)
    wait_all(arriving[5:])
    terms[...] = jnp.dot(grad_pre, tokens[...], preferred_element_type=F32).astype(BF)


def gradient(length, gathered, along, along_f, wd, *saved):
    quarter, features = wd.shape
    pool = gathered.shape[0] // SPAN
    count = 8 * length
    return call(
        functools.partial(gradient_body, length),
        (jax.ShapeDtypeStruct((quarter, features), BF), jax.ShapeDtypeStruct((8, 128), F32)),
        [WHOLE] * 3 + [IN_HBM] * 7,
        [
            pltpu.VMEM(gathered.shape, F32),
            pltpu.VMEM((pool, features), F32),
            pltpu.VMEM((pool, features), F32),
            pltpu.VMEM((quarter, features), BF),
            pltpu.VMEM((2, quarter, count // 2), BF),
            pltpu.VMEM((count, features), BF),
            pltpu.VMEM((count, features), BF),
            pltpu.SemaphoreType.DMA((7,)),
        ],
    )(gathered, along, along_f, *in_hbm(wd, *saved))


def add_near_body(own_rows, arrived, loss, out):
    senders, rows, features = arrived.shape
    total = arrived[0].astype(F32)
    for s in range(1, senders):
        total = total + arrived[s].astype(F32)
    groups = rows // own_rows
    spread = lax.broadcasted_iota(jnp.int32, (groups * 8, rows), 0)
    source = lax.broadcasted_iota(jnp.int32, (groups * 8, rows), 1)
    group = spread >> 3
    inner = spread & 7
    pick = ((inner < own_rows) & (source == own_rows * group + inner)).astype(F32).astype(BF)
    placed = jnp.dot(pick, total.astype(BF), preferred_element_type=F32)
    first, second, third = split(loss[0:1, 0:1])
    lane = lax.broadcasted_iota(jnp.int32, (1, features), 1)
    pieces = jnp.where(lane == 0, first, jnp.where(lane == 1, second, jnp.where(lane == 2, third, 0.0)))
    is_loss = (lax.broadcasted_iota(jnp.int32, (groups * 8, 1), 0) & 7) == own_rows
    out[...] = jnp.where(is_loss, pieces, placed).astype(BF)


def add_near(arrived, loss, own_rows):
    groups = arrived.shape[1] // own_rows
    return call(
        functools.partial(add_near_body, own_rows),
        jax.ShapeDtypeStruct((groups * 8, arrived.shape[2]), BF),
        [WHOLE] * 2,
    )(arrived, loss)


def add_far_body(count, arrived, rows, mean_loss):
    total = arrived[0].astype(F32)
    for s in range(1, arrived.shape[0]):
        total = total + arrived[s].astype(F32)
    own = rows.shape[0]
    rows[...] = total[:own]
    loss = arrived[0, own : own + 1, 0:128].astype(F32) + arrived[1, own : own + 1, 0:128].astype(F32)
    lane = lax.broadcasted_iota(jnp.int32, (1, 128), 1)
    mean_loss[...] = jnp.sum(jnp.where(lane < 3, loss, 0.0), -1, keepdims=True) * (1.0 / count)


def add_far(arrived, own_rows, count):
    return call(
        functools.partial(add_far_body, count),
        (
            jax.ShapeDtypeStruct((own_rows, arrived.shape[2]), F32),
            jax.ShapeDtypeStruct((1, 1), F32),
        ),
        [WHOLE],
    )(arrived)


def exchange(tiles, axes):
    return lax.all_to_all(tiles, axes, split_axis=0, concat_axis=0, tiled=True)


def step(q_hidden, p_hidden, w_up, w_down, pos_index, hard_index):
    features = w_up.shape[1]
    q = q_hidden.reshape(-1, features)
    p = p_hidden.reshape(-1, features)
    near, far = "y", ("z", "xh")
    near_count = lax.axis_size(near)
    far_count = lax.axis_size(far)
    own_rows = w_up.shape[0] // (4 * near_count * far_count)
    peers = lax.axis_size(("y", "xl", "z"))
    qx = lax.ppermute(q, "xl", SWAP)
    px = lax.ppermute(p, "xl", SWAP)
    indices = (pos_index, hard_index.reshape(1, -1))
    message, shared = encode(q, p, w_up, w_down, indices, peers)
    gathered = exchange(message, ("y", "xl", "z"))
    shared_s = lax.ppermute(shared, "c", SWAP)
    shared_x = encode(qx, px, w_up, w_down)
    shared_xs = lax.ppermute(shared_x, "c", SWAP)
    slope, tokens, normed, wd, along, wu_mine, wd_mine = prepare_near(
        near_count, shared, shared_s, w_up, w_down
    )
    slope_f, tokens_f, normed_f, along_f = prepare_far(shared_x, shared_xs, wu_mine, wd_mine)
    gathered = lax.all_gather(gathered, "c", axis=0, tiled=True)
    terms, loss = gradient(
        q.shape[0], gathered.reshape(-1, 128), along, along_f, wd, slope, slope_f, tokens, tokens_f, normed, normed_f
    )
    arrived = exchange(terms.reshape(near_count, -1, features), near)
    partial = add_near(arrived, loss, own_rows)
    arrived = exchange(partial.reshape(far_count, 8, features), far)
    count = lax.axis_size(DP) * lax.axis_size("xh")
    rows, mean_loss = add_far(arrived, own_rows, count)
    return rows, mean_loss.reshape(())


def solution(mesh):
    finer = Mesh(mesh.devices.reshape(4, 2, 8, 2, mesh.shape["rep"]), ("y", "xl", "z", "c", "xh"))
    return jax.shard_map(
        step,
        mesh=finer,
        in_specs=(
            P("xh", DP, None, None),
            P("xh", DP, None, None),
            P(),
            P(),
            P("xh", DP),
            P("xh", DP, None),
        ),
        out_specs=(P((*DP, "xh"), None), P()),
        check_vma=False,
    )
```
